64 devices in a mesh: data: 4 (over x, y), cp: 16 (over z, core).
Axes of the slice: x: 2, y: 2, z: 8, core: 2. Of those that a mesh axis runs over, the one named last changes fastest.
The devices are a block of a 4x4x8 slice.
Arguments:
- q: bfloat16 [4, 4096, 8, 256], P('data', 'cp'), parts along dimension 0
- k: bfloat16 [4, 4096, 8, 256], P('data', 'cp'), parts along dimension 0
- v: bfloat16 [4, 4096, 8, 256], P('data', 'cp'), parts along dimension 0
- o: bfloat16 [4, 4096, 8, 256], P('data', 'cp'), parts along dimension 0
- lse: float32 [4, 8, 4096], P('data', None, 'cp'), parts along dimension 0
- do: bfloat16 [4, 4096, 8, 256], P('data', 'cp'), parts along dimension 0
Outputs:
- output 1: bfloat16 [4, 4096, 8, 256], P('data', 'cp'), parts along dimension 0
- output 2: bfloat16 [4, 4096, 8, 256], P('data', 'cp'), parts along dimension 0
- output 3: bfloat16 [4, 4096, 8, 256], P('data', 'cp'), parts along dimension 0
There are 4 independent parts. The reference program is written for one: setup_inputs(seed, part) draws one part's arguments, and reference() takes and returns one part's arrays. A program takes and returns all parts, laid end to end along the dimension named above; each array names one.
All inputs are finite; a program needn't handle non-finite values.
Results may differ from the reference program's by a relative error of at most 0.001.
Values are sent between devices in bfloat16 or wider.
A program may use at most 768 MiB of HBM per device.

```python
import jax
import jax.numpy as jnp
from jax import lax
import numpy as np

CP = 16
BATCH = 1
TOKENS_DEV = 256
HEADS = 8
HEAD = 256


def _positions():
    c = TOKENS_DEV // 2
    dev = np.arange(CP)[:, None]
    u = np.arange(c)[None, :]
    return np.concatenate([dev * c + u, (2 * CP - 1 - dev) * c + u], axis=1).reshape(2 * CP, c)


def _segments(x):
    c = TOKENS_DEV // 2
    return jnp.moveaxis(x.astype(jnp.float32).reshape(BATCH, 2 * CP, c, HEADS, HEAD), 1, 0)


def _forward(q, k, v):
    c = TOKENS_DEV // 2
    scale = HEAD ** -0.5
    pos = jnp.asarray(_positions(), dtype=jnp.int32)
    qs, ks, vs = _segments(q), _segments(k), _segments(v)

    def one(xs):
        qb, pq = xs

        def scores(kb, pk):
            s = jnp.einsum('bqhd,bkhd->bhqk', qb, kb) * scale
            return jnp.where(pq[:, None] >= pk[None, :], s, -jnp.inf)

        def stat(carry, ys):
            m, l = carry
            s = scores(*ys)
            m2 = jnp.maximum(m, jnp.max(s, axis=-1))
            return (m2, l * jnp.exp(m - m2) + jnp.sum(jnp.exp(s - m2[..., None]), axis=-1)), None

        m0 = jnp.full((BATCH, HEADS, c), -jnp.inf, jnp.float32)
        (m, l), _ = lax.scan(stat, (m0, jnp.zeros_like(m0)), (ks, pos))
        lse = m + jnp.log(l)

        def acc(o, ys):
            kb, vb, pk = ys
            p = jnp.exp(scores(kb, pk) - lse[..., None])
            return o + jnp.einsum('bhqk,bkhd->bqhd', p, vb), None

        o, _ = lax.scan(acc, jnp.zeros((BATCH, c, HEADS, HEAD), jnp.float32), (ks, vs, pos))
        return o, lse

    o, lse = lax.map(one, (qs, pos))
    o = jnp.moveaxis(o, 0, 1).reshape(BATCH, CP * TOKENS_DEV, HEADS, HEAD).astype(jnp.bfloat16)
    lse = jnp.moveaxis(lse, 0, 2).reshape(BATCH, HEADS, CP * TOKENS_DEV)
    return o, lse


def setup_inputs(seed: int = 0, part: int = 0) -> dict:
    key = jax.random.fold_in(jax.random.PRNGKey(seed), part)
    kq, kk, kv, kd = jax.random.split(key, 4)
    shape = (BATCH, CP * TOKENS_DEV, HEADS, HEAD)
    q = jax.random.normal(kq, shape, jnp.float32).astype(jnp.bfloat16)
    k = jax.random.normal(kk, shape, jnp.float32).astype(jnp.bfloat16)
    v = jax.random.normal(kv, shape, jnp.float32).astype(jnp.bfloat16)
    do = jax.random.normal(kd, shape, jnp.float32).astype(jnp.bfloat16)
    o, lse = _forward(q, k, v)
    return {'q': q, 'k': k, 'v': v, 'o': o, 'lse': lse, 'do': do}


def reference(q, k, v, o, lse, do):
    nseg = 2 * CP
    c = TOKENS_DEV // 2
    scale = HEAD ** -0.5
    pos = jnp.asarray(_positions(), dtype=jnp.int32)
    qs, ks, vs, dos = _segments(q), _segments(k), _segments(v), _segments(do)
    delta = jnp.sum(do.astype(jnp.float32) * o.astype(jnp.float32), axis=-1)
    deltas = jnp.moveaxis(jnp.swapaxes(delta, 1, 2).reshape(BATCH, HEADS, nseg, c), 2, 0)
    lses = jnp.moveaxis(lse.reshape(BATCH, HEADS, nseg, c), 2, 0)

    def per_query(carry, xs):
        dk, dv = carry
        qb, dob, lb, db, pq = xs

        def per_key(ys):
            kb, vb, pk = ys
            s = jnp.einsum('bqhd,bkhd->bhqk', qb, kb) * scale
            p = jnp.where(pq[:, None] >= pk[None, :], jnp.exp(s - lb[..., None]), 0.0)
            dvb = jnp.einsum('bhqk,bqhd->bkhd', p.astype(jnp.bfloat16).astype(jnp.float32), dob)
            dp = jnp.einsum('bqhd,bkhd->bhqk', dob, vb)
            ds = (p * (dp - db[..., None])).astype(jnp.bfloat16).astype(jnp.float32)
            return jnp.einsum('bhqk,bkhd->bqhd', ds, kb), jnp.einsum('bhqk,bqhd->bkhd', ds, qb), dvb

        dqs, dks, dvs = lax.map(per_key, (ks, vs, pos))
        return (dk + dks, dv + dvs), jnp.sum(dqs, axis=0)

    zero = jnp.zeros_like(ks)
    (dk, dv), dq = lax.scan(per_query, (zero, zero), (qs, dos, lses, deltas, pos))

    def unseg(x):
        return jnp.moveaxis(x, 0, 1).reshape(BATCH, CP * TOKENS_DEV, HEADS, HEAD).astype(jnp.bfloat16)

    return unseg(dq * scale), unseg(dk * scale), unseg(dv)
```

```python
import functools

import jax
import jax.numpy as jnp
from jax import lax
from jax.experimental import pallas as pl
from jax.experimental.pallas import tpu as pltpu
from jax.sharding import PartitionSpec as P

F32 = jnp.float32
BF16 = jnp.bfloat16
MESH = pl.DeviceIdType.MESH
EARLY, LATE = 0, 1
K, V, Q, DO, O = range(5)


def _dot(a, b):
    return jnp.dot(a, b, preferred_element_type=F32)


def _dot_nt(a, b):
    return lax.dot_general(a, b, (((1,), (1,)), ((), ())), preferred_element_type=F32)


def _kernel(n, q_h, k_h, v_h, o_h, do_h, lse_h, dq_h, dk_h, dv_h,
            raw, lse_v, wide, send, ldsend, kv, qd, ld, kt, dqt, dqx, dkv, outs, outr, outv,
            load_sem, lse_sem, store_sem, kv_s, kv_r, qd_s, qd_r, ld_s, ld_r,
            fw_s, fw_r, fl_s, fl_r, dx_s, dx_r, og_s, og_r, oq_s, oq_r):
    chips = n // 2
    tokens, heads, dim = raw.shape[1:]
    c = tokens // 2
    lanes = wide.shape[-1]
    scale = dim ** -0.5
    me = lax.axis_index('cp')
    z = me // 2
    core = me % 2
    sib = me + 1 - 2 * core
    around = list(range(chips // 2, 0, -1))
    around = [d for k in around for d in ([k] if 2 * k == chips else [k, chips - k])]

    def peer(chip):
        return {'cp': 2 * chip + core}

    barrier = pltpu.get_barrier_semaphore()
    for d in range(1, chips):
        pl.semaphore_signal(barrier, inc=1, device_id=peer((z + d) % chips), device_id_type=MESH)
    pl.semaphore_signal(barrier, inc=1, device_id={'cp': sib}, device_id_type=MESH)

    hbm = {K: k_h, V: v_h, Q: q_h, DO: do_h, O: o_h}

    def load(t, half):
        rows = pl.ds(half * c, c)
        return pltpu.make_async_copy(hbm[t].at[rows], raw.at[t, rows], load_sem.at[t, half])

    for half in (LATE, EARLY):
        for t in (K, V, Q, DO, O):
            load(t, half).start()
    lse_load = pltpu.make_async_copy(lse_h, lse_v, lse_sem)
    lse_load.start()

    def spread(x):
        for l in range(dim // lanes):
            wide[l] = x[:, :, l * lanes:(l + 1) * lanes].reshape(c * heads, lanes)

    def head_rows(h):
        return pl.ds(h, c, stride=heads)

    def relayout(t, half, wait=True):
        if wait:
            load(t, half).wait()
        spread(raw[t, pl.ds(half * c, c)].astype(F32))
        for h in range(heads):
            for l in range(dim // lanes):
                send[half, t, h, :, pl.ds(l * lanes, lanes)] = wide[l, head_rows(h), :].astype(BF16)

    def copy_kv(half, d, slot):
        head = (z + d) % chips
        src, dst = send.at[half, pl.ds(K, 2), head], kv.at[half, :, slot]
        if d == 0:
            return pltpu.make_async_copy(src, dst, kv_r.at[half, slot])
        return pltpu.make_async_remote_copy(src, dst, kv_s.at[half, d], kv_r.at[half, slot],
                                            device_id=peer(head), device_id_type=MESH)

    def copy_qd(half, d, slot):
        head = (z + d) % chips
        src, dst = send.at[half, pl.ds(Q, 2), head], qd.at[half, :, 2 * slot + core]
        if d == 0:
            return pltpu.make_async_copy(src, dst, qd_r.at[half, slot])
        return pltpu.make_async_remote_copy(src, dst, qd_s.at[half, d], qd_r.at[half, slot],
                                            device_id=peer(head), device_id_type=MESH)

    def copy_ld(d, slot):
        head = (z + d) % chips
        src, dst = ldsend.at[head], ld.at[2 * slot + core]
        if d == 0:
            return pltpu.make_async_copy(src, dst, ld_r.at[slot])
        return pltpu.make_async_remote_copy(src, dst, ld_s.at[d], ld_r.at[slot],
                                            device_id=peer(head), device_id_type=MESH)

    def forward_qd(half, slot, parity):
        ref = qd.at[half, :, 2 * slot + parity]
        return pltpu.make_async_remote_copy(ref, ref, fw_s.at[half, slot], fw_r.at[half, slot],
                                            device_id={'cp': sib}, device_id_type=MESH)

    def forward_ld(slot, parity):
        ref = ld.at[2 * slot + parity]
        return pltpu.make_async_remote_copy(ref, ref, fl_s.at[slot], fl_r.at[slot],
                                            device_id={'cp': sib}, device_id_type=MESH)

    def exchange_dq(half):
        return pltpu.make_async_remote_copy(dqt.at[half, :, 1 - core], dqx.at[half], dx_s.at[half], dx_r.at[half],
                                            device_id={'cp': sib}, device_id_type=MESH)

    def copy_dkv(half, d, slot):
        chip = (z + d) % chips
        src, dst = outs.at[half, pl.ds(0, 2), chip], outr.at[half, pl.ds(0, 2), slot]
        if d == 0:
            return pltpu.make_async_copy(src, dst, og_r.at[half, slot])
        return pltpu.make_async_remote_copy(src, dst, og_s.at[half, d], og_r.at[half, slot],
                                            device_id=peer(chip), device_id_type=MESH)

    def copy_dq(half, d, slot):
        chip = (z + d) % chips
        src, dst = outs.at[half, 2, chip], outr.at[half, 2, slot]
        if d == 0:
            return pltpu.make_async_copy(src, dst, oq_r.at[half, slot])
        return pltpu.make_async_remote_copy(src, dst, oq_s.at[half, d], oq_r.at[half, slot],
                                            device_id=peer(chip), device_id_type=MESH)

    def start_all(make):
        for d in around + [0]:
            make(d, z).start()

    def wait_from(make, d):
        if d == 0:
            make(0, z).wait()
        else:
            make(d, (z - d + chips) % chips).wait_recv()

    def wait_sent(make):
        for d in around:
            make(d, z).wait_send()

    relayout(K, LATE)
    relayout(V, LATE)
    pl.semaphore_wait(barrier, chips)
    start_all(functools.partial(copy_kv, LATE))
    relayout(Q, LATE)
    relayout(DO, LATE)
    start_all(functools.partial(copy_qd, LATE))
    lse_load.wait()
    for half in (LATE, EARLY):
        load(O, half).wait()
        if half == EARLY:
            load(DO, half).wait()
        rows = pl.ds(half * c, c)
        spread(raw[DO, rows].astype(F32) * raw[O, rows].astype(F32))
        for h in range(heads):
            prod = sum(wide[l, head_rows(h), :] for l in range(dim // lanes))
            ldsend[h, pl.ds(2 + half, 1), :] = jnp.sum(prod.T, axis=0, keepdims=True)
            ldsend[h, pl.ds(half, 1), :] = lse_v[pl.ds(h, 1), pl.ds(half * c, c)]
    start_all(copy_ld)

    relayout(K, EARLY)
    relayout(V, EARLY)
    start_all(functools.partial(copy_kv, EARLY))
    relayout(Q, EARLY)
    relayout(DO, EARLY, wait=False)
    start_all(functools.partial(copy_qd, EARLY))

    def clear(s, carry):
        for half in range(2):
            for p in range(2):
                dqt[half, s, p] = jnp.zeros((dim, c), F32)
                dkv[half, p, s] = jnp.zeros((c, dim), F32)
        return carry

    lax.fori_loop(0, chips, clear, 0)

    def tile(kh, qh, i, j, width, masked):
        k = kv[kh, 0, pl.ds(2 * i, 2)].reshape(2 * c, dim)
        v = kv[kh, 1, pl.ds(2 * i, 2)].reshape(2 * c, dim)
        first = width * j
        q = qd[qh, 0, pl.ds(first, width)].reshape(width * c, dim)
        do = qd[qh, 1, pl.ds(first, width)].reshape(width * c, dim)
        lse = jnp.concatenate([ld[first + w, pl.ds(qh, 1), :] for w in range(width)], axis=1)
        delta = jnp.concatenate([ld[first + w, pl.ds(2 + qh, 1), :] for w in range(width)], axis=1)
        p = jnp.exp(_dot_nt(k, q) * scale - lse)
        if masked:
            sign = 1 if kh == EARLY else -1
            row = lax.broadcasted_iota(jnp.int32, (2 * c, width * c), 0)
            col = lax.broadcasted_iota(jnp.int32, (2 * c, width * c), 1)
            kpos = jnp.where(row >= c, row - c + sign * 2 * c, row) + sign * (4 * i + core) * c
            qpos = jnp.where(col >= c, col - c + sign * c, col) + sign * first * c
            p = jnp.where(qpos >= kpos, p, 0.0)
        rows = pl.ds(2 * i, 2)
        dkv[kh, 1, rows] += _dot(p.astype(BF16), do).reshape(2, c, dim)
        ds = (p * (_dot_nt(v, do) - delta)).astype(BF16)
        dkv[kh, 0, rows] += _dot(ds, q).reshape(2, c, dim)
        dq = _dot(kt[...], ds)
        for w in range(width):
            dqt[qh, width // 2 * j + w // 2, w % 2] += dq[:, w * c:(w + 1) * c]

    def sweep(kh, qh, lo, hi, width, masked):
        def outer(i, carry):
            kt[...] = kv[kh, 0, pl.ds(2 * i, 2)].reshape(2 * c, dim).T

            def inner(j, carry):
                tile(kh, qh, i, j, width, masked)
                return carry

            lax.fori_loop(lo(i), hi(i), inner, 0)
            return carry

        lax.fori_loop(0, chips // 2, outer, 0)

    def receive_qd(half):
        for d in [0] + around[::-1]:
            wait_from(functools.partial(copy_qd, half), d)
            forward_qd(half, (z - d + chips) % chips, core).start()

    def receive_forwarded(half):
        for s in range(chips):
            forward_qd(half, s, 1 - core).wait_recv()

    def receive_kv(half):
        for d in [0] + around:
            wait_from(functools.partial(copy_kv, half), d)

    def round_dkv(half):
        def one(s, carry):
            outs[half, 0, s] = (dkv[half, 0, s] * scale).astype(BF16)
            outs[half, 1, s] = dkv[half, 1, s].astype(BF16)
            return carry

        lax.fori_loop(0, chips, one, 0)

    def round_dq(half):
        def one(s, carry):
            outs[half, 2, s] = ((dqt[half, s, core] + dqx[half, s]) * scale).astype(BF16).T
            return carry

        lax.fori_loop(0, chips, one, 0)

    receive_qd(LATE)
    for d in [0] + around:
        wait_from(copy_ld, d)
        forward_ld((z - d + chips) % chips, core).start()
    receive_kv(LATE)
    receive_forwarded(LATE)
    for s in range(chips):
        forward_ld(s, 1 - core).wait_recv()
    sweep(LATE, LATE, lambda i: 0, lambda i: 2 * i + 2, 2, True)
    round_dkv(LATE)
    start_all(functools.partial(copy_dkv, LATE))

    receive_kv(EARLY)
    sweep(EARLY, LATE, lambda i: 0, lambda i: chips // 2, 4, False)
    exchange_dq(LATE).start()
    receive_qd(EARLY)
    exchange_dq(LATE).wait()
    round_dq(LATE)
    start_all(functools.partial(copy_dq, LATE))

    receive_forwarded(EARLY)
    sweep(EARLY, EARLY, lambda i: 2 * i, lambda i: chips, 2, True)
    round_dkv(EARLY)
    exchange_dq(EARLY).start()
    start_all(functools.partial(copy_dkv, EARLY))
    exchange_dq(EARLY).wait()
    round_dq(EARLY)
    start_all(functools.partial(copy_dq, EARLY))

    out = {0: dk_h, 1: dv_h, 2: dq_h}

    def store(t, half):
        rows = pl.ds(half * c, c)
        return pltpu.make_async_copy(outv.at[t, rows], out[t].at[rows], store_sem.at[t, half])

    def deliver(t, half):
        for h in range(heads):
            for l in range(dim // lanes):
                wide[l, head_rows(h), :] = outr[half, t, h, :, pl.ds(l * lanes, lanes)].astype(F32)
        for l in range(dim // lanes):
            outv[t, pl.ds(half * c, c), :, pl.ds(l * lanes, lanes)] = wide[l].reshape(c, heads, lanes).astype(BF16)
        store(t, half).start()

    for half in (LATE, EARLY):
        for d in [0] + around[::-1]:
            wait_from(functools.partial(copy_dkv, half), d)
        deliver(0, half)
        deliver(1, half)
        for d in [0] + around[::-1]:
            wait_from(functools.partial(copy_dq, half), d)
        deliver(2, half)

    for half in (LATE, EARLY):
        for make in (copy_kv, copy_qd, copy_dkv, copy_dq):
            wait_sent(functools.partial(make, half))
        for s in range(chips):
            forward_qd(half, s, core).wait_send()
        for t in range(3):
            store(t, half).wait()
    wait_sent(copy_ld)
    for s in range(chips):
        forward_ld(s, core).wait_send()


def solution(mesh):
    n = mesh.shape['cp']
    spec = P('data', 'cp', None, None)
    lspec = P('data', None, 'cp')

    def local(q, k, v, o, lse, do):
        batch, tokens, heads, dim = q.shape
        chips = n // 2
        assert batch == 1 and heads == chips
        c = tokens // 2
        dma = pltpu.SemaphoreType.DMA
        args = [x.reshape(tokens, heads, dim) for x in (q, k, v, o, do)] + [lse.reshape(heads, tokens)]
        outs = pl.pallas_call(
            functools.partial(_kernel, n),
            out_shape=[jax.ShapeDtypeStruct((tokens, heads, dim), BF16)] * 3,
            in_specs=[pl.BlockSpec(memory_space=pl.ANY)] * 6,
            out_specs=[pl.BlockSpec(memory_space=pl.ANY)] * 3,
            scratch_shapes=[
                pltpu.VMEM((5, tokens, heads, dim), BF16),
                pltpu.VMEM((heads, tokens), F32),
                pltpu.VMEM((dim // 128, c * heads, 128), F32),
                pltpu.VMEM((2, 4, heads, c, dim), BF16),
                pltpu.VMEM((heads, 4, c), F32),
                pltpu.VMEM((2, 2, chips, c, dim), BF16),
                pltpu.VMEM((2, 2, n, c, dim), BF16),
                pltpu.VMEM((n, 4, c), F32),
                pltpu.VMEM((dim, 2 * c), BF16),
                pltpu.VMEM((2, chips, 2, dim, c), F32),
                pltpu.VMEM((2, chips, dim, c), F32),
                pltpu.VMEM((2, 2, chips, c, dim), F32),
                pltpu.VMEM((2, 3, chips, c, dim), BF16),
                pltpu.VMEM((2, 3, heads, c, dim), BF16),
                pltpu.VMEM((3, tokens, heads, dim), BF16),
                dma((5, 2)), dma, dma((3, 2)),
                dma((2, chips)), dma((2, chips)), dma((2, chips)), dma((2, chips)), dma((chips,)), dma((chips,)),
                dma((2, chips)), dma((2, chips)), dma((chips,)), dma((chips,)), dma((2,)), dma((2,)),
                dma((2, chips)), dma((2, chips)), dma((2, chips)), dma((2, chips)),
            ],
            compiler_params=pltpu.CompilerParams(collective_id=0, has_side_effects=True,
                                                 vmem_limit_bytes=60 * 1024 * 1024),
            name='attention_backward',
        )(*args)
        dk, dv, dq = outs[1], outs[2], outs[0]
        return tuple(x.reshape(batch, tokens, heads, dim) for x in (dq, dk, dv))

    return jax.shard_map(local, mesh=mesh, in_specs=(spec, spec, spec, spec, lspec, spec),
                         out_specs=(spec, spec, spec), check_vma=False)
```

```python
import functools

import jax
import jax.numpy as jnp
from jax import lax
from jax.experimental import pallas as pl
from jax.experimental.pallas import tpu as pltpu
from jax.sharding import PartitionSpec as P

F32 = jnp.float32
BF16 = jnp.bfloat16
MESH = pl.DeviceIdType.MESH
EARLY, LATE = 0, 1
K, V, Q, DO, O = range(5)


def _dot(a, b):
    return jnp.dot(a, b, preferred_element_type=F32)


def _dot_nt(a, b):
    return lax.dot_general(a, b, (((1,), (1,)), ((), ())), preferred_element_type=F32)


def _kernel(n, q_h, k_h, v_h, o_h, do_h, lse_h, outv,
            raw, lse_v, wide, send, ldsend, kv, qd, ld, kt, dqt, dqx, dkv, outs, outr,
            tokens_up, tokens_down, load_sem, lse_sem, kv_s, kv_r, qd_s, qd_r, ld_s, ld_r,
            fw_s, fw_r, fl_s, fl_r, dx_s, dx_r, og_s, og_r, oq_s, oq_r):
    chips = n // 2
    tokens, heads, dim = raw.shape[1:]
    c = tokens // 2
    lanes = wide.shape[-1]
    scale = dim ** -0.5
    me = lax.axis_index('cp')
    z = me // 2
    core = me % 2
    sib = me + 1 - 2 * core
    around = list(range(chips // 2, 0, -1))
    around = [d for k in around for d in ([k] if 2 * k == chips else [k, chips - k])]

    def peer(chip):
        return {'cp': 2 * chip + core}

    barrier = pltpu.get_barrier_semaphore()
    above, below = peer((z + 1) % chips), peer((z + chips - 1) % chips)
    for near in (above, below):
        pl.semaphore_signal(barrier, inc=1, device_id=near, device_id_type=MESH)
    pl.semaphore_signal(barrier, inc=1, device_id={'cp': sib}, device_id_type=MESH)

    hbm = {K: k_h, V: v_h, Q: q_h, DO: do_h, O: o_h}

    def load(t, half):
        rows = pl.ds(half * c, c)
        return pltpu.make_async_copy(hbm[t].at[rows], raw.at[t, rows], load_sem.at[t, half])

    load(K, LATE).start()
    load(V, LATE).start()

    pl.semaphore_wait(barrier, 3)

    def pass_on(k):
        pl.semaphore_signal(tokens_up.at[k], inc=1, device_id=above, device_id_type=MESH)
        pl.semaphore_signal(tokens_down.at[k], inc=1, device_id=below, device_id_type=MESH)

    def hear(k):
        pl.semaphore_wait(tokens_up.at[k], 1)
        pl.semaphore_wait(tokens_down.at[k], 1)

    pass_on(1)
    for t in (Q, DO, O):
        load(t, LATE).start()
    for t in (K, V, Q, DO, O):
        load(t, EARLY).start()
    lse_load = pltpu.make_async_copy(lse_h, lse_v, lse_sem)
    lse_load.start()

    def spread(x):
        for l in range(dim // lanes):
            wide[0, l] = x[:, :, l * lanes:(l + 1) * lanes].reshape(c * heads, lanes)

    def head_rows(h):
        return pl.ds(h, c, stride=heads)

    def relayout(t, half, wait=True):
        if wait:
            load(t, half).wait()
        spread(raw[t, pl.ds(half * c, c)].astype(F32))
        for h in range(heads):
            for l in range(dim // lanes):
                send[half, t, h, :, pl.ds(l * lanes, lanes)] = wide[0, l, head_rows(h), :].astype(BF16)

    def copy_kv(half, d, slot):
        head = (z + d) % chips
        src, dst = send.at[half, pl.ds(K, 2), head], kv.at[half, :, slot]
        if d == 0:
            return pltpu.make_async_copy(src, dst, kv_r.at[half, slot])
        return pltpu.make_async_remote_copy(src, dst, kv_s.at[half, d], kv_r.at[half, slot],
                                            device_id=peer(head), device_id_type=MESH)

    def copy_qd(half, d, slot):
        head = (z + d) % chips
        src, dst = send.at[half, pl.ds(Q, 2), head], qd.at[half, :, 2 * slot + core]
        if d == 0:
            return pltpu.make_async_copy(src, dst, qd_r.at[half, slot])
        return pltpu.make_async_remote_copy(src, dst, qd_s.at[half, d], qd_r.at[half, slot],
                                            device_id=peer(head), device_id_type=MESH)

    def copy_ld(d, slot):
        head = (z + d) % chips
        src, dst = ldsend.at[head], ld.at[2 * slot + core]
        if d == 0:
            return pltpu.make_async_copy(src, dst, ld_r.at[slot])
        return pltpu.make_async_remote_copy(src, dst, ld_s.at[d], ld_r.at[slot],
                                            device_id=peer(head), device_id_type=MESH)

    def forward_qd(half, slot, parity):
        ref = qd.at[half, :, 2 * slot + parity]
        return pltpu.make_async_remote_copy(ref, ref, fw_s.at[half, slot], fw_r.at[half, slot],
                                            device_id={'cp': sib}, device_id_type=MESH)

    def forward_ld(slot, parity):
        ref = ld.at[2 * slot + parity]
        return pltpu.make_async_remote_copy(ref, ref, fl_s.at[slot], fl_r.at[slot],
                                            device_id={'cp': sib}, device_id_type=MESH)

    def exchange_dq(half):
        return pltpu.make_async_remote_copy(dqt.at[half, :, 1 - core], dqx.at[half], dx_s.at[half], dx_r.at[half],
                                            device_id={'cp': sib}, device_id_type=MESH)

    def copy_dkv(half, d, slot):
        chip = (z + d) % chips
        src, dst = outs.at[half, pl.ds(0, 2), chip], outr.at[half, pl.ds(0, 2), slot]
        if d == 0:
            return pltpu.make_async_copy(src, dst, og_r.at[half, slot])
        return pltpu.make_async_remote_copy(src, dst, og_s.at[half, d], og_r.at[half, slot],
                                            device_id=peer(chip), device_id_type=MESH)

    def copy_dq(half, d, slot):
        chip = (z + d) % chips
        src, dst = outs.at[half, 2, chip], outr.at[half, 2, slot]
        if d == 0:
            return pltpu.make_async_copy(src, dst, oq_r.at[half, slot])
        return pltpu.make_async_remote_copy(src, dst, oq_s.at[half, d], oq_r.at[half, slot],
                                            device_id=peer(chip), device_id_type=MESH)

    def start_all(make):
        for d in around + [0]:
            make(d, z).start()

    def wait_from(make, d):
        if d == 0:
            make(0, z).wait()
        else:
            make(d, (z - d + chips) % chips).wait_recv()

    def wait_sent(make):
        for d in around:
            make(d, z).wait_send()

    relayout(K, LATE)
    relayout(V, LATE)
    copy_kv(LATE, 0, z).start()
    for k in range(1, chips // 2 + 1):
        if k > 1:
            hear(k - 1)
            if k < chips // 2:
                pass_on(k)
        for d in around[::-1]:
            if min(d, chips - d) == k:
                copy_kv(LATE, d, z).start()
    relayout(Q, LATE)
    relayout(DO, LATE)
    start_all(functools.partial(copy_qd, LATE))
    lse_load.wait()
    for half in (LATE, EARLY):
        load(O, half).wait()
        if half == EARLY:
            load(DO, half).wait()
        rows = pl.ds(half * c, c)
        spread(raw[DO, rows].astype(F32) * raw[O, rows].astype(F32))
        for h in range(heads):
            prod = sum(wide[0, l, head_rows(h), :] for l in range(dim // lanes))
            ldsend[h, pl.ds(2 + half, 1), :] = jnp.sum(prod.T, axis=0, keepdims=True)
            ldsend[h, pl.ds(half, 1), :] = lse_v[pl.ds(h, 1), pl.ds(half * c, c)]
    start_all(copy_ld)

    relayout(K, EARLY)
    relayout(V, EARLY)
    start_all(functools.partial(copy_kv, EARLY))
    relayout(Q, EARLY)
    relayout(DO, EARLY, wait=False)
    start_all(functools.partial(copy_qd, EARLY))

    def clear(s, carry):
        for half in range(2):
            for p in range(2):
                dqt[half, s, p] = jnp.zeros((dim, c), F32)
                dkv[half, p, s] = jnp.zeros((c, dim), F32)
        return carry

    lax.fori_loop(0, chips, clear, 0)

    def tile(kh, qh, i, j, width, masked):
        k = kv[kh, 0, pl.ds(2 * i, 2)].reshape(2 * c, dim)
        v = kv[kh, 1, pl.ds(2 * i, 2)].reshape(2 * c, dim)
        first = width * j
        q = qd[qh, 0, pl.ds(first, width)].reshape(width * c, dim)
        do = qd[qh, 1, pl.ds(first, width)].reshape(width * c, dim)
        lse = jnp.concatenate([ld[first + w, pl.ds(qh, 1), :] for w in range(width)], axis=1)
        delta = jnp.concatenate([ld[first + w, pl.ds(2 + qh, 1), :] for w in range(width)], axis=1)
        p = jnp.exp(_dot_nt(k, q) * scale - lse)
        if masked:
            sign = 1 if kh == EARLY else -1
            row = lax.broadcasted_iota(jnp.int32, (2 * c, width * c), 0)
            col = lax.broadcasted_iota(jnp.int32, (2 * c, width * c), 1)
            kpos = jnp.where(row >= c, row - c + sign * 2 * c, row) + sign * (4 * i + core) * c
            qpos = jnp.where(col >= c, col - c + sign * c, col) + sign * first * c
            p = jnp.where(qpos >= kpos, p, 0.0)
        rows = pl.ds(2 * i, 2)
        dkv[kh, 1, rows] += _dot(p.astype(BF16), do).reshape(2, c, dim)
        ds = (p * (_dot_nt(v, do) - delta)).astype(BF16)
        dkv[kh, 0, rows] += _dot(ds, q).reshape(2, c, dim)
        dq = _dot(kt[...], ds)
        for w in range(width):
            dqt[qh, width // 2 * j + w // 2, w % 2] += dq[:, w * c:(w + 1) * c]

    def sweep(kh, qh, lo, hi, width, masked):
        def outer(i, carry):
            kt[...] = kv[kh, 0, pl.ds(2 * i, 2)].reshape(2 * c, dim).T

            def inner(j, carry):
                tile(kh, qh, i, j, width, masked)
                return carry

            lax.fori_loop(lo(i), hi(i), inner, 0)
            return carry

        lax.fori_loop(0, chips // 2, outer, 0)

    def receive_qd(half):
        for d in [0] + around[::-1]:
            wait_from(functools.partial(copy_qd, half), d)
            forward_qd(half, (z - d + chips) % chips, core).start()

    def receive_forwarded(half):
        for s in range(chips):
            forward_qd(half, s, 1 - core).wait_recv()

    def receive_kv(half):
        for d in [0] + around:
            wait_from(functools.partial(copy_kv, half), d)

    def round_dkv(half):
        def one(s, carry):
            outs[half, 0, s] = (dkv[half, 0, s] * scale).astype(BF16)
            outs[half, 1, s] = dkv[half, 1, s].astype(BF16)
            return carry

        lax.fori_loop(0, chips, one, 0)

    def round_dq(half):
        def one(s, carry):
            outs[half, 2, s] = ((dqt[half, s, core] + dqx[half, s]) * scale).astype(BF16).T
            return carry

        lax.fori_loop(0, chips, one, 0)

    receive_qd(LATE)
    for d in [0] + around:
        wait_from(copy_ld, d)
        forward_ld((z - d + chips) % chips, core).start()
    receive_kv(LATE)
    receive_forwarded(LATE)
    for s in range(chips):
        forward_ld(s, 1 - core).wait_recv()
    sweep(LATE, LATE, lambda i: 0, lambda i: 2 * i + 2, 2, True)
    round_dkv(LATE)
    start_all(functools.partial(copy_dkv, LATE))

    receive_kv(EARLY)
    sweep(EARLY, LATE, lambda i: 0, lambda i: chips // 2, 4, False)
    exchange_dq(LATE).start()
    receive_qd(EARLY)
    exchange_dq(LATE).wait()
    round_dq(LATE)
    start_all(functools.partial(copy_dq, LATE))

    receive_forwarded(EARLY)
    sweep(EARLY, EARLY, lambda i: 2 * i, lambda i: chips, 2, True)
    round_dkv(EARLY)
    exchange_dq(EARLY).start()
    start_all(functools.partial(copy_dkv, EARLY))
    exchange_dq(EARLY).wait()
    round_dq(EARLY)
    start_all(functools.partial(copy_dq, EARLY))

    def gather(make, half, ts):
        for d in [0] + around:
            wait_from(functools.partial(make, half), d)
            h = (z - d + chips) % chips
            for t in ts:
                for l in range(dim // lanes):
                    wide[t, l, head_rows(h), :] = outr[half, t, h, :, pl.ds(l * lanes, lanes)].astype(F32)
        for t in ts:
            for l in range(dim // lanes):
                outv[t, pl.ds(half * c, c), :, pl.ds(l * lanes, lanes)] = (
                    wide[t, l].reshape(c, heads, lanes).astype(BF16))

    for half in (LATE, EARLY):
        gather(copy_dkv, half, (0, 1))
        gather(copy_dq, half, (2,))

    for half in (LATE, EARLY):
        for make in (copy_kv, copy_qd, copy_dkv, copy_dq):
            wait_sent(functools.partial(make, half))
        for s in range(chips):
            forward_qd(half, s, core).wait_send()
    wait_sent(copy_ld)
    for s in range(chips):
        forward_ld(s, core).wait_send()


def _write(x, dk, dv, dq, sem):
    copies = [pltpu.make_async_copy(x.at[t], out, sem.at[t]) for t, out in enumerate((dk, dv, dq))]
    for copy in copies:
        copy.start()
    for copy in copies:
        copy.wait()


def solution(mesh):
    n = mesh.shape['cp']
    spec = P('data', 'cp', None, None)
    lspec = P('data', None, 'cp')

    def local(q, k, v, o, lse, do):
        batch, tokens, heads, dim = q.shape
        chips = n // 2
        assert batch == 1 and heads == chips
        c = tokens // 2
        dma = pltpu.SemaphoreType.DMA
        args = [x.reshape(tokens, heads, dim) for x in (q, k, v, o, do)] + [lse.reshape(heads, tokens)]
        grads = pl.pallas_call(
            functools.partial(_kernel, n),
            out_shape=pltpu.VMEM((3, tokens, heads, dim), BF16),
            in_specs=[pl.BlockSpec(memory_space=pl.ANY)] * 6,
            out_specs=pl.BlockSpec(memory_space=pltpu.VMEM),
            scratch_shapes=[
                pltpu.VMEM((5, tokens, heads, dim), BF16),
                pltpu.VMEM((heads, tokens), F32),
                pltpu.VMEM((3, dim // 128, c * heads, 128), F32),
                pltpu.VMEM((2, 4, heads, c, dim), BF16),
                pltpu.VMEM((heads, 4, c), F32),
                pltpu.VMEM((2, 2, chips, c, dim), BF16),
                pltpu.VMEM((2, 2, n, c, dim), BF16),
                pltpu.VMEM((n, 4, c), F32),
                pltpu.VMEM((dim, 2 * c), BF16),
                pltpu.VMEM((2, chips, 2, dim, c), F32),
                pltpu.VMEM((2, chips, dim, c), F32),
                pltpu.VMEM((2, 2, chips, c, dim), F32),
                pltpu.VMEM((2, 3, chips, c, dim), BF16),
                pltpu.VMEM((2, 3, heads, c, dim), BF16),
                pltpu.SemaphoreType.REGULAR((chips // 2,)), pltpu.SemaphoreType.REGULAR((chips // 2,)),
                dma((5, 2)), dma,
                dma((2, chips)), dma((2, chips)), dma((2, chips)), dma((2, chips)), dma((chips,)), dma((chips,)),
                dma((2, chips)), dma((2, chips)), dma((chips,)), dma((chips,)), dma((2,)), dma((2,)),
                dma((2, chips)), dma((2, chips)), dma((2, chips)), dma((2, chips)),
            ],
            compiler_params=pltpu.CompilerParams(collective_id=0, has_side_effects=True,
                                                 vmem_limit_bytes=56 * 1024 * 1024),
            name='attention_backward',
        )(*args)
        dk, dv, dq = pl.pallas_call(
            _write,
            out_shape=[jax.ShapeDtypeStruct((tokens, heads, dim), BF16)] * 3,
            in_specs=[pl.BlockSpec(memory_space=pltpu.VMEM)],
            out_specs=[pl.BlockSpec(memory_space=pl.ANY)] * 3,
            scratch_shapes=[dma((3,))],
            compiler_params=pltpu.CompilerParams(vmem_limit_bytes=8 * 1024 * 1024),
            name='write_gradients',
        )(pltpu.with_memory_space_constraint(grads, pltpu.VMEM))
        return tuple(x.reshape(batch, tokens, heads, dim) for x in (dq, dk, dv))

    return jax.shard_map(local, mesh=mesh, in_specs=(spec, spec, spec, spec, lspec, spec),
                         out_specs=(spec, spec, spec), check_vma=False)
```

```python
import functools

import jax
import jax.numpy as jnp
from jax import lax
from jax.experimental import pallas as pl
from jax.experimental.pallas import tpu as pltpu
from jax.sharding import PartitionSpec as P

F32 = jnp.float32
BF16 = jnp.bfloat16
MESH = pl.DeviceIdType.MESH
EARLY, LATE = 0, 1
K, V, Q, DO, O = range(5)


def _dot(a, b):
    return jnp.dot(a, b, preferred_element_type=F32)


def _dot_nt(a, b):
    return lax.dot_general(a, b, (((1,), (1,)), ((), ())), preferred_element_type=F32)


def _kernel(n, q_h, k_h, v_h, o_h, do_h, lse_h, outv,
            raw, lse_v, wide, send, ldsend, kv, qd, ld, kt, dqt, dqx, dkv, outs, outr,
            tokens_up, tokens_down, load_sem, lse_sem, kv_s, kv_r, qd_s, qd_r, ld_s, ld_r,
            fw_s, fw_r, fl_s, fl_r, dx_s, dx_r, og_s, og_r, oq_s, oq_r):
    chips = n // 2
    tokens, heads, dim = raw.shape[1:]
    c = tokens // 2
    lanes = wide.shape[-1]
    scale = dim ** -0.5
    me = lax.axis_index('cp')
    z = me // 2
    core = me % 2
    sib = me + 1 - 2 * core
    around = [d for k in range(1, chips // 2) for d in (k, chips - k)] + [chips // 2]

    def peer(chip):
        return {'cp': 2 * chip + core}

    barrier = pltpu.get_barrier_semaphore()
    above, below = peer((z + 1) % chips), peer((z + chips - 1) % chips)
    for near in (above, below):
        pl.semaphore_signal(barrier, inc=1, device_id=near, device_id_type=MESH)
    pl.semaphore_signal(barrier, inc=1, device_id={'cp': sib}, device_id_type=MESH)

    hbm = {K: k_h, V: v_h, Q: q_h, DO: do_h, O: o_h}

    def load(t, half):
        rows = pl.ds(half * c, c)
        return pltpu.make_async_copy(hbm[t].at[rows], raw.at[t, rows], load_sem.at[t, half])

    load(K, LATE).start()
    load(V, LATE).start()

    pl.semaphore_wait(barrier, 3)

    def pass_on(k):
        pl.semaphore_signal(tokens_up.at[k], inc=1, device_id=above, device_id_type=MESH)
        pl.semaphore_signal(tokens_down.at[k], inc=1, device_id=below, device_id_type=MESH)

    def hear(k):
        pl.semaphore_wait(tokens_up.at[k], 1)
        pl.semaphore_wait(tokens_down.at[k], 1)

    pass_on(1)
    for t in (Q, DO, O):
        load(t, LATE).start()
    for t in (K, V, Q, DO, O):
        load(t, EARLY).start()
    lse_load = pltpu.make_async_copy(lse_h, lse_v, lse_sem)
    lse_load.start()

    def spread(x):
        for l in range(dim // lanes):
            wide[0, l] = x[:, :, l * lanes:(l + 1) * lanes].reshape(c * heads, lanes)

    def head_rows(h):
        return pl.ds(h, c, stride=heads)

    def relayout(t, half, wait=True):
        if wait:
            load(t, half).wait()
        spread(raw[t, pl.ds(half * c, c)].astype(F32))
        for h in range(heads):
            for l in range(dim // lanes):
                send[half, t, h, :, pl.ds(l * lanes, lanes)] = wide[0, l, head_rows(h), :].astype(BF16)

    def copy_kv(half, d, slot):
        head = (z + d) % chips
        src, dst = send.at[half, pl.ds(K, 2), head], kv.at[half, :, slot]
        if isinstance(d, int) and d == 0:
            return pltpu.make_async_copy(src, dst, kv_r.at[half, slot])
        return pltpu.make_async_remote_copy(src, dst, kv_s.at[half, d], kv_r.at[half, slot],
                                            device_id=peer(head), device_id_type=MESH)

    def copy_qd(half, d, slot):
        head = (z + d) % chips
        src, dst = send.at[half, pl.ds(Q, 2), head], qd.at[half, :, 2 * slot + core]
        if isinstance(d, int) and d == 0:
            return pltpu.make_async_copy(src, dst, qd_r.at[half, slot])
        return pltpu.make_async_remote_copy(src, dst, qd_s.at[half, d], qd_r.at[half, slot],
                                            device_id=peer(head), device_id_type=MESH)

    def copy_ld(d, slot):
        head = (z + d) % chips
        src, dst = ldsend.at[head], ld.at[2 * slot + core]
        if isinstance(d, int) and d == 0:
            return pltpu.make_async_copy(src, dst, ld_r.at[slot])
        return pltpu.make_async_remote_copy(src, dst, ld_s.at[d], ld_r.at[slot],
                                            device_id=peer(head), device_id_type=MESH)

    def forward_qd(half, slot, parity):
        ref = qd.at[half, :, 2 * slot + parity]
        return pltpu.make_async_remote_copy(ref, ref, fw_s.at[half, slot], fw_r.at[half, slot],
                                            device_id={'cp': sib}, device_id_type=MESH)

    def forward_ld(slot, parity):
        ref = ld.at[2 * slot + parity]
        return pltpu.make_async_remote_copy(ref, ref, fl_s.at[slot], fl_r.at[slot],
                                            device_id={'cp': sib}, device_id_type=MESH)

    def exchange_dq(half):
        return pltpu.make_async_remote_copy(dqt.at[half, :, 1 - core], dqx.at[half], dx_s.at[half], dx_r.at[half],
                                            device_id={'cp': sib}, device_id_type=MESH)

    def copy_dkv(half, d, slot):
        chip = (z + d) % chips
        src, dst = outs.at[half, pl.ds(0, 2), chip], outr.at[half, pl.ds(0, 2), slot]
        if isinstance(d, int) and d == 0:
            return pltpu.make_async_copy(src, dst, og_r.at[half, slot])
        return pltpu.make_async_remote_copy(src, dst, og_s.at[half, d], og_r.at[half, slot],
                                            device_id=peer(chip), device_id_type=MESH)

    def copy_dq(half, d, slot):
        chip = (z + d) % chips
        src, dst = outs.at[half, 2, chip], outr.at[half, 2, slot]
        if isinstance(d, int) and d == 0:
            return pltpu.make_async_copy(src, dst, oq_r.at[half, slot])
        return pltpu.make_async_remote_copy(src, dst, oq_s.at[half, d], oq_r.at[half, slot],
                                            device_id=peer(chip), device_id_type=MESH)

    def start_all(make):
        for d in [0] + around:
            make(d, z).start()

    def start_all_low_first(make):
        @pl.when(z == 0)
        def _():
            make(0, z).start()

        @pl.when(z != 0)
        def _():
            make(chips - z, z).start()

        for d in [0] + around:
            @pl.when((z + d) % chips != 0)
            def _():
                make(d, z).start()

    def wait_from(make, d):
        if d == 0:
            make(0, z).wait()
        else:
            make(d, (z - d + chips) % chips).wait_recv()

    def wait_sent(make):
        for d in around:
            make(d, z).wait_send()

    relayout(K, LATE)
    relayout(V, LATE)
    copy_kv(LATE, 0, z).start()
    for k in range(1, chips // 2 + 1):
        if k > 1:
            hear(k - 1)
            if k < chips // 2:
                pass_on(k)
        for d in around:
            if min(d, chips - d) == k:
                copy_kv(LATE, d, z).start()
    relayout(Q, LATE)
    relayout(DO, LATE)
    start_all(functools.partial(copy_qd, LATE))
    lse_load.wait()
    for half in (LATE, EARLY):
        load(O, half).wait()
        if half == EARLY:
            load(DO, half).wait()
        rows = pl.ds(half * c, c)
        spread(raw[DO, rows].astype(F32) * raw[O, rows].astype(F32))
        for h in range(heads):
            prod = sum(wide[0, l, head_rows(h), :] for l in range(dim // lanes))
            ldsend[h, pl.ds(2 + half, 1), :] = jnp.sum(prod.T, axis=0, keepdims=True)
            ldsend[h, pl.ds(half, 1), :] = lse_v[pl.ds(h, 1), pl.ds(half * c, c)]
    start_all(copy_ld)

    relayout(K, EARLY)
    relayout(V, EARLY)
    start_all(functools.partial(copy_kv, EARLY))
    relayout(Q, EARLY)
    relayout(DO, EARLY, wait=False)
    start_all(functools.partial(copy_qd, EARLY))

    def clear(s, carry):
        for half in range(2):
            for p in range(2):
                dqt[half, s, p] = jnp.zeros((dim, c), F32)
                dkv[half, p, s] = jnp.zeros((c, dim), F32)
        return carry

    lax.fori_loop(0, chips, clear, 0)

    def tile(kh, qh, i, j, width, masked):
        k = kv[kh, 0, pl.ds(2 * i, 2)].reshape(2 * c, dim)
        v = kv[kh, 1, pl.ds(2 * i, 2)].reshape(2 * c, dim)
        first = width * j
        q = qd[qh, 0, pl.ds(first, width)].reshape(width * c, dim)
        do = qd[qh, 1, pl.ds(first, width)].reshape(width * c, dim)
        lse = jnp.concatenate([ld[first + w, pl.ds(qh, 1), :] for w in range(width)], axis=1)
        delta = jnp.concatenate([ld[first + w, pl.ds(2 + qh, 1), :] for w in range(width)], axis=1)
        p = jnp.exp(_dot_nt(k, q) * scale - lse)
        if masked:
            sign = 1 if kh == EARLY else -1
            row = lax.broadcasted_iota(jnp.int32, (2 * c, width * c), 0)
            col = lax.broadcasted_iota(jnp.int32, (2 * c, width * c), 1)
            kpos = jnp.where(row >= c, row - c + sign * 2 * c, row) + sign * (4 * i + core) * c
            qpos = jnp.where(col >= c, col - c + sign * c, col) + sign * first * c
            p = jnp.where(qpos >= kpos, p, 0.0)
        rows = pl.ds(2 * i, 2)
        dkv[kh, 1, rows] += _dot(p.astype(BF16), do).reshape(2, c, dim)
        ds = (p * (_dot_nt(v, do) - delta)).astype(BF16)
        dkv[kh, 0, rows] += _dot(ds, q).reshape(2, c, dim)
        dq = _dot(kt[...], ds)
        for w in range(width):
            dqt[qh, width // 2 * j + w // 2, w % 2] += dq[:, w * c:(w + 1) * c]

    def sweep(kh, qh, lo, hi, width, masked):
        def outer(i, carry):
            kt[...] = kv[kh, 0, pl.ds(2 * i, 2)].reshape(2 * c, dim).T

            def inner(j, carry):
                tile(kh, qh, i, j, width, masked)
                return carry

            lax.fori_loop(lo(i), hi(i), inner, 0)
            return carry

        lax.fori_loop(0, chips // 2, outer, 0)

    def receive_qd(half):
        for d in [0] + around:
            wait_from(functools.partial(copy_qd, half), d)
            forward_qd(half, (z - d + chips) % chips, core).start()

    def receive_forwarded(half):
        for s in range(chips):
            forward_qd(half, s, 1 - core).wait_recv()

    def receive_kv(half):
        for d in [0] + around:
            wait_from(functools.partial(copy_kv, half), d)

    def round_dkv(half):
        def one(s, carry):
            outs[half, 0, s] = (dkv[half, 0, s] * scale).astype(BF16)
            outs[half, 1, s] = dkv[half, 1, s].astype(BF16)
            return carry

        lax.fori_loop(0, chips, one, 0)

    def round_dq(half):
        def one(s, carry):
            outs[half, 2, s] = ((dqt[half, s, core] + dqx[half, s]) * scale).astype(BF16).T
            return carry

        lax.fori_loop(0, chips, one, 0)

    receive_qd(LATE)
    for d in [0] + around:
        wait_from(copy_ld, d)
        forward_ld((z - d + chips) % chips, core).start()
    receive_kv(LATE)
    receive_forwarded(LATE)
    for s in range(chips):
        forward_ld(s, 1 - core).wait_recv()
    sweep(LATE, LATE, lambda i: 0, lambda i: 2 * i + 2, 2, True)
    round_dkv(LATE)
    start_all(functools.partial(copy_dkv, LATE))

    receive_kv(EARLY)
    sweep(EARLY, LATE, lambda i: 0, lambda i: chips // 2, 4, False)
    exchange_dq(LATE).start()
    receive_qd(EARLY)
    exchange_dq(LATE).wait()
    round_dq(LATE)
    start_all(functools.partial(copy_dq, LATE))

    receive_forwarded(EARLY)
    sweep(EARLY, EARLY, lambda i: 2 * i, lambda i: chips, 2, True)
    round_dkv(EARLY)
    exchange_dq(EARLY).start()
    start_all(functools.partial(copy_dkv, EARLY))
    exchange_dq(EARLY).wait()
    round_dq(EARLY)
    start_all_low_first(functools.partial(copy_dq, EARLY))

    def gather(make, half, ts):
        for d in [0] + around:
            wait_from(functools.partial(make, half), d)
            h = (z - d + chips) % chips
            for t in ts:
                for l in range(dim // lanes):
                    wide[t, l, head_rows(h), :] = outr[half, t, h, :, pl.ds(l * lanes, lanes)].astype(F32)
        for t in ts:
            for l in range(dim // lanes):
                outv[t, pl.ds(half * c, c), :, pl.ds(l * lanes, lanes)] = (
                    wide[t, l].reshape(c, heads, lanes).astype(BF16))

    for half in (LATE, EARLY):
        gather(copy_dkv, half, (0, 1))
        gather(copy_dq, half, (2,))

    for half in (LATE, EARLY):
        for make in (copy_kv, copy_qd, copy_dkv, copy_dq):
            wait_sent(functools.partial(make, half))
        for s in range(chips):
            forward_qd(half, s, core).wait_send()
    wait_sent(copy_ld)
    for s in range(chips):
        forward_ld(s, core).wait_send()


def _write(x, dk, dv, dq, sem):
    copies = [pltpu.make_async_copy(x.at[t], out, sem.at[t]) for t, out in enumerate((dk, dv, dq))]
    for copy in copies:
        copy.start()
    for copy in copies:
        copy.wait()


def solution(mesh):
    n = mesh.shape['cp']
    spec = P('data', 'cp', None, None)
    lspec = P('data', None, 'cp')

    def local(q, k, v, o, lse, do):
        batch, tokens, heads, dim = q.shape
        chips = n // 2
        assert batch == 1 and heads == chips
        c = tokens // 2
        dma = pltpu.SemaphoreType.DMA
        args = [x.reshape(tokens, heads, dim) for x in (q, k, v, o, do)] + [lse.reshape(heads, tokens)]
        grads = pl.pallas_call(
            functools.partial(_kernel, n),
            out_shape=pltpu.VMEM((3, tokens, heads, dim), BF16),
            in_specs=[pl.BlockSpec(memory_space=pl.ANY)] * 6,
            out_specs=pl.BlockSpec(memory_space=pltpu.VMEM),
            scratch_shapes=[
                pltpu.VMEM((5, tokens, heads, dim), BF16),
                pltpu.VMEM((heads, tokens), F32),
                pltpu.VMEM((3, dim // 128, c * heads, 128), F32),
                pltpu.VMEM((2, 4, heads, c, dim), BF16),
                pltpu.VMEM((heads, 4, c), F32),
                pltpu.VMEM((2, 2, chips, c, dim), BF16),
                pltpu.VMEM((2, 2, n, c, dim), BF16),
                pltpu.VMEM((n, 4, c), F32),
                pltpu.VMEM((dim, 2 * c), BF16),
                pltpu.VMEM((2, chips, 2, dim, c), F32),
                pltpu.VMEM((2, chips, dim, c), F32),
                pltpu.VMEM((2, 2, chips, c, dim), F32),
                pltpu.VMEM((2, 3, chips, c, dim), BF16),
                pltpu.VMEM((2, 3, heads, c, dim), BF16),
                pltpu.SemaphoreType.REGULAR((chips // 2,)), pltpu.SemaphoreType.REGULAR((chips // 2,)),
                dma((5, 2)), dma,
                dma((2, chips)), dma((2, chips)), dma((2, chips)), dma((2, chips)), dma((chips,)), dma((chips,)),
                dma((2, chips)), dma((2, chips)), dma((chips,)), dma((chips,)), dma((2,)), dma((2,)),
                dma((2, chips)), dma((2, chips)), dma((2, chips)), dma((2, chips)),
            ],
            compiler_params=pltpu.CompilerParams(collective_id=0, has_side_effects=True,
                                                 vmem_limit_bytes=56 * 1024 * 1024),
            name='attention_backward',
        )(*args)
        dk, dv, dq = pl.pallas_call(
            _write,
            out_shape=[jax.ShapeDtypeStruct((tokens, heads, dim), BF16)] * 3,
            in_specs=[pl.BlockSpec(memory_space=pltpu.VMEM)],
            out_specs=[pl.BlockSpec(memory_space=pl.ANY)] * 3,
            scratch_shapes=[dma((3,))],
            compiler_params=pltpu.CompilerParams(vmem_limit_bytes=8 * 1024 * 1024),
            name='write_gradients',
        )(pltpu.with_memory_space_constraint(grads, pltpu.VMEM))
        return tuple(x.reshape(batch, tokens, heads, dim) for x in (dq, dk, dv))

    return jax.shard_map(local, mesh=mesh, in_specs=(spec, spec, spec, spec, lspec, spec),
                         out_specs=(spec, spec, spec), check_vma=False)
```

```python
import functools

import jax
import jax.numpy as jnp
from jax import lax
from jax.experimental import pallas as pl
from jax.experimental.pallas import tpu as pltpu
from jax.sharding import PartitionSpec as P

F32 = jnp.float32
BF16 = jnp.bfloat16
MESH = pl.DeviceIdType.MESH
EARLY, LATE = 0, 1
K, V, Q, DO, O = range(5)


def _dot(a, b):
    return jnp.dot(a, b, preferred_element_type=F32)


def _dot_nt(a, b):
    return lax.dot_general(a, b, (((1,), (1,)), ((), ())), preferred_element_type=F32)


def _kernel(n, q_h, k_h, v_h, o_h, do_h, lse_h, outv,
            raw, lse_v, wide, send, ldsend, kv, qd, ld, kt, dqt, dqx, dkv, outs, outr,
            tokens_up, tokens_down, load_sem, lse_sem, kv_s, kv_r, qd_s, qd_r, ld_s, ld_r,
            fw_s, fw_r, fl_s, fl_r, dx_s, dx_r, og_s, og_r, oq_s, oq_r):
    chips = n // 2
    tokens, heads, dim = raw.shape[1:]
    c = tokens // 2
    lanes = wide.shape[-1]
    scale = dim ** -0.5
    me = lax.axis_index('cp')
    z = me // 2
    core = me % 2
    sib = me + 1 - 2 * core
    around = [d for k in range(1, chips // 2) for d in (chips - k, k)] + [chips // 2]

    def peer(chip):
        return {'cp': 2 * chip + core}

    barrier = pltpu.get_barrier_semaphore()
    above, below = peer((z + 1) % chips), peer((z + chips - 1) % chips)
    for near in (above, below):
        pl.semaphore_signal(barrier, inc=1, device_id=near, device_id_type=MESH)
    pl.semaphore_signal(barrier, inc=1, device_id={'cp': sib}, device_id_type=MESH)

    hbm = {K: k_h, V: v_h, Q: q_h, DO: do_h, O: o_h}

    def load(t, half):
        rows = pl.ds(half * c, c)
        return pltpu.make_async_copy(hbm[t].at[rows], raw.at[t, rows], load_sem.at[t, half])

    load(K, LATE).start()
    load(V, LATE).start()

    pl.semaphore_wait(barrier, 3)

    def pass_on(k):
        pl.semaphore_signal(tokens_up.at[k], inc=1, device_id=above, device_id_type=MESH)
        pl.semaphore_signal(tokens_down.at[k], inc=1, device_id=below, device_id_type=MESH)

    def hear(k):
        pl.semaphore_wait(tokens_up.at[k], 1)
        pl.semaphore_wait(tokens_down.at[k], 1)

    pass_on(1)
    for t in (Q, DO, O):
        load(t, LATE).start()
    for t in (K, V, Q, DO, O):
        load(t, EARLY).start()
    lse_load = pltpu.make_async_copy(lse_h, lse_v, lse_sem)
    lse_load.start()

    def spread(x):
        for l in range(dim // lanes):
            wide[0, l] = x[:, :, l * lanes:(l + 1) * lanes].reshape(c * heads, lanes)

    def head_rows(h):
        return pl.ds(h, c, stride=heads)

    def relayout(t, half, wait=True):
        if wait:
            load(t, half).wait()
        spread(raw[t, pl.ds(half * c, c)].astype(F32))
        for h in range(heads):
            for l in range(dim // lanes):
                send[half, t, h, :, pl.ds(l * lanes, lanes)] = wide[0, l, head_rows(h), :].astype(BF16)

    def copy_kv(half, d, slot):
        head = (z + d) % chips
        src, dst = send.at[half, pl.ds(K, 2), head], kv.at[half, :, slot]
        if isinstance(d, int) and d == 0:
            return pltpu.make_async_copy(src, dst, kv_r.at[half, slot])
        return pltpu.make_async_remote_copy(src, dst, kv_s.at[half, d], kv_r.at[half, slot],
                                            device_id=peer(head), device_id_type=MESH)

    def copy_qd(half, d, slot):
        head = (z + d) % chips
        src, dst = send.at[half, pl.ds(Q, 2), head], qd.at[half, :, 2 * slot + core]
        if isinstance(d, int) and d == 0:
            return pltpu.make_async_copy(src, dst, qd_r.at[half, slot])
        return pltpu.make_async_remote_copy(src, dst, qd_s.at[half, d], qd_r.at[half, slot],
                                            device_id=peer(head), device_id_type=MESH)

    def copy_ld(d, slot):
        head = (z + d) % chips
        src, dst = ldsend.at[head], ld.at[2 * slot + core]
        if isinstance(d, int) and d == 0:
            return pltpu.make_async_copy(src, dst, ld_r.at[slot])
        return pltpu.make_async_remote_copy(src, dst, ld_s.at[d], ld_r.at[slot],
                                            device_id=peer(head), device_id_type=MESH)

    def forward_qd(half, slot, parity):
        ref = qd.at[half, :, 2 * slot + parity]
        return pltpu.make_async_remote_copy(ref, ref, fw_s.at[half, slot], fw_r.at[half, slot],
                                            device_id={'cp': sib}, device_id_type=MESH)

    def forward_ld(slot, parity):
        ref = ld.at[2 * slot + parity]
        return pltpu.make_async_remote_copy(ref, ref, fl_s.at[slot], fl_r.at[slot],
                                            device_id={'cp': sib}, device_id_type=MESH)

    def exchange_dq(half):
        return pltpu.make_async_remote_copy(dqt.at[half, :, 1 - core], dqx.at[half], dx_s.at[half], dx_r.at[half],
                                            device_id={'cp': sib}, device_id_type=MESH)

    def copy_dkv(half, d, slot):
        chip = (z + d) % chips
        src, dst = outs.at[half, pl.ds(0, 2), chip], outr.at[half, pl.ds(0, 2), slot]
        if isinstance(d, int) and d == 0:
            return pltpu.make_async_copy(src, dst, og_r.at[half, slot])
        return pltpu.make_async_remote_copy(src, dst, og_s.at[half, d], og_r.at[half, slot],
                                            device_id=peer(chip), device_id_type=MESH)

    def copy_dq(half, d, slot):
        chip = (z + d) % chips
        src, dst = outs.at[half, 2, chip], outr.at[half, 2, slot]
        if isinstance(d, int) and d == 0:
            return pltpu.make_async_copy(src, dst, oq_r.at[half, slot])
        return pltpu.make_async_remote_copy(src, dst, oq_s.at[half, d], oq_r.at[half, slot],
                                            device_id=peer(chip), device_id_type=MESH)

    def start_all(make):
        for d in [0] + around:
            make(d, z).start()

    def start_all_low_first(make):
        @pl.when(z == 0)
        def _():
            make(0, z).start()

        @pl.when(z != 0)
        def _():
            make(chips - z, z).start()

        for d in [0] + around:
            @pl.when((z + d) % chips != 0)
            def _():
                make(d, z).start()

    def wait_from(make, d):
        if d == 0:
            make(0, z).wait()
        else:
            make(d, (z - d + chips) % chips).wait_recv()

    def wait_sent(make):
        for d in around:
            make(d, z).wait_send()

    relayout(K, LATE)
    relayout(V, LATE)
    copy_kv(LATE, 0, z).start()
    for k in range(1, chips // 2 + 1):
        if k > 1:
            hear(k - 1)
            if k < chips // 2:
                pass_on(k)
        for d in around:
            if min(d, chips - d) == k:
                copy_kv(LATE, d, z).start()
    relayout(Q, LATE)
    relayout(DO, LATE)
    start_all(functools.partial(copy_qd, LATE))
    lse_load.wait()
    for half in (LATE, EARLY):
        load(O, half).wait()
        if half == EARLY:
            load(DO, half).wait()
        rows = pl.ds(half * c, c)
        spread(raw[DO, rows].astype(F32) * raw[O, rows].astype(F32))
        for h in range(heads):
            prod = sum(wide[0, l, head_rows(h), :] for l in range(dim // lanes))
            ldsend[h, pl.ds(2 + half, 1), :] = jnp.sum(prod.T, axis=0, keepdims=True)
            ldsend[h, pl.ds(half, 1), :] = lse_v[pl.ds(h, 1), pl.ds(half * c, c)]
    start_all(copy_ld)

    relayout(K, EARLY)
    relayout(V, EARLY)
    start_all(functools.partial(copy_kv, EARLY))
    relayout(Q, EARLY)
    relayout(DO, EARLY, wait=False)
    start_all(functools.partial(copy_qd, EARLY))

    def clear(s, carry):
        for half in range(2):
            for p in range(2):
                dqt[half, s, p] = jnp.zeros((dim, c), F32)
                dkv[half, p, s] = jnp.zeros((c, dim), F32)
        return carry

    lax.fori_loop(0, chips, clear, 0)

    def tile(kh, qh, i, j, width, masked):
        k = kv[kh, 0, pl.ds(2 * i, 2)].reshape(2 * c, dim)
        v = kv[kh, 1, pl.ds(2 * i, 2)].reshape(2 * c, dim)
        first = width * j
        q = qd[qh, 0, pl.ds(first, width)].reshape(width * c, dim)
        do = qd[qh, 1, pl.ds(first, width)].reshape(width * c, dim)
        lse = jnp.concatenate([ld[first + w, pl.ds(qh, 1), :] for w in range(width)], axis=1)
        delta = jnp.concatenate([ld[first + w, pl.ds(2 + qh, 1), :] for w in range(width)], axis=1)
        p = jnp.exp(_dot_nt(k, q) * scale - lse)
        if masked:
            sign = 1 if kh == EARLY else -1
            row = lax.broadcasted_iota(jnp.int32, (2 * c, width * c), 0)
            col = lax.broadcasted_iota(jnp.int32, (2 * c, width * c), 1)
            kpos = jnp.where(row >= c, row - c + sign * 2 * c, row) + sign * (4 * i + core) * c
            qpos = jnp.where(col >= c, col - c + sign * c, col) + sign * first * c
            p = jnp.where(qpos >= kpos, p, 0.0)
        rows = pl.ds(2 * i, 2)
        dkv[kh, 1, rows] += _dot(p.astype(BF16), do).reshape(2, c, dim)
        ds = (p * (_dot_nt(v, do) - delta)).astype(BF16)
        dkv[kh, 0, rows] += _dot(ds, q).reshape(2, c, dim)
        dq = _dot(kt[...], ds)
        for w in range(width):
            dqt[qh, width // 2 * j + w // 2, w % 2] += dq[:, w * c:(w + 1) * c]

    def sweep(kh, qh, lo, hi, width, masked):
        def outer(i, carry):
            kt[...] = kv[kh, 0, pl.ds(2 * i, 2)].reshape(2 * c, dim).T

            def inner(j, carry):
                tile(kh, qh, i, j, width, masked)
                return carry

            lax.fori_loop(lo(i), hi(i), inner, 0)
            return carry

        lax.fori_loop(0, chips // 2, outer, 0)

    def receive_qd(half):
        for d in [0] + around:
            wait_from(functools.partial(copy_qd, half), d)
            forward_qd(half, (z - d + chips) % chips, core).start()

    def receive_forwarded(half):
        for s in range(chips):
            forward_qd(half, s, 1 - core).wait_recv()

    def receive_kv(half):
        for d in [0] + around:
            wait_from(functools.partial(copy_kv, half), d)

    def round_dkv(half):
        def one(s, carry):
            outs[half, 0, s] = (dkv[half, 0, s] * scale).astype(BF16)
            outs[half, 1, s] = dkv[half, 1, s].astype(BF16)
            return carry

        lax.fori_loop(0, chips, one, 0)

    def round_dq(half):
        def one(s, carry):
            outs[half, 2, s] = ((dqt[half, s, core] + dqx[half, s]) * scale).astype(BF16).T
            return carry

        lax.fori_loop(0, chips, one, 0)

    receive_qd(LATE)
    for d in [0] + around:
        wait_from(copy_ld, d)
        forward_ld((z - d + chips) % chips, core).start()
    receive_kv(LATE)
    receive_forwarded(LATE)
    for s in range(chips):
        forward_ld(s, 1 - core).wait_recv()
    sweep(LATE, LATE, lambda i: 0, lambda i: 2 * i + 2, 2, True)
    round_dkv(LATE)
    start_all(functools.partial(copy_dkv, LATE))

    receive_kv(EARLY)
    sweep(EARLY, LATE, lambda i: 0, lambda i: chips // 2, 4, False)
    exchange_dq(LATE).start()
    receive_qd(EARLY)
    exchange_dq(LATE).wait()
    round_dq(LATE)
    start_all(functools.partial(copy_dq, LATE))

    receive_forwarded(EARLY)
    sweep(EARLY, EARLY, lambda i: 2 * i, lambda i: chips, 2, True)
    round_dkv(EARLY)
    exchange_dq(EARLY).start()
    start_all(functools.partial(copy_dkv, EARLY))
    exchange_dq(EARLY).wait()
    round_dq(EARLY)
    start_all_low_first(functools.partial(copy_dq, EARLY))

    def gather(make, half, ts):
        for d in [0] + around:
            wait_from(functools.partial(make, half), d)
            h = (z - d + chips) % chips
            for t in ts:
                for l in range(dim // lanes):
                    wide[t, l, head_rows(h), :] = outr[half, t, h, :, pl.ds(l * lanes, lanes)].astype(F32)
        for t in ts:
            for l in range(dim // lanes):
                outv[t, pl.ds(half * c, c), :, pl.ds(l * lanes, lanes)] = (
                    wide[t, l].reshape(c, heads, lanes).astype(BF16))

    for half in (LATE, EARLY):
        gather(copy_dkv, half, (0, 1))
        gather(copy_dq, half, (2,))

    for half in (LATE, EARLY):
        for make in (copy_kv, copy_qd, copy_dkv, copy_dq):
            wait_sent(functools.partial(make, half))
        for s in range(chips):
            forward_qd(half, s, core).wait_send()
    wait_sent(copy_ld)
    for s in range(chips):
        forward_ld(s, core).wait_send()


def _write(x, dk, dv, dq, sem):
    copies = [pltpu.make_async_copy(x.at[t], out, sem.at[t]) for t, out in enumerate((dk, dv, dq))]
    for copy in copies:
        copy.start()
    for copy in copies:
        copy.wait()


def solution(mesh):
    n = mesh.shape['cp']
    spec = P('data', 'cp', None, None)
    lspec = P('data', None, 'cp')

    def local(q, k, v, o, lse, do):
        batch, tokens, heads, dim = q.shape
        chips = n // 2
        assert batch == 1 and heads == chips
        c = tokens // 2
        dma = pltpu.SemaphoreType.DMA
        args = [x.reshape(tokens, heads, dim) for x in (q, k, v, o, do)] + [lse.reshape(heads, tokens)]
        grads = pl.pallas_call(
            functools.partial(_kernel, n),
            out_shape=pltpu.VMEM((3, tokens, heads, dim), BF16),
            in_specs=[pl.BlockSpec(memory_space=pl.ANY)] * 6,
            out_specs=pl.BlockSpec(memory_space=pltpu.VMEM),
            scratch_shapes=[
                pltpu.VMEM((5, tokens, heads, dim), BF16),
                pltpu.VMEM((heads, tokens), F32),
                pltpu.VMEM((3, dim // 128, c * heads, 128), F32),
                pltpu.VMEM((2, 4, heads, c, dim), BF16),
                pltpu.VMEM((heads, 4, c), F32),
                pltpu.VMEM((2, 2, chips, c, dim), BF16),
                pltpu.VMEM((2, 2, n, c, dim), BF16),
                pltpu.VMEM((n, 4, c), F32),
                pltpu.VMEM((dim, 2 * c), BF16),
                pltpu.VMEM((2, chips, 2, dim, c), F32),
                pltpu.VMEM((2, chips, dim, c), F32),
                pltpu.VMEM((2, 2, chips, c, dim), F32),
                pltpu.VMEM((2, 3, chips, c, dim), BF16),
                pltpu.VMEM((2, 3, heads, c, dim), BF16),
                pltpu.SemaphoreType.REGULAR((chips // 2,)), pltpu.SemaphoreType.REGULAR((chips // 2,)),
                dma((5, 2)), dma,
                dma((2, chips)), dma((2, chips)), dma((2, chips)), dma((2, chips)), dma((chips,)), dma((chips,)),
                dma((2, chips)), dma((2, chips)), dma((chips,)), dma((chips,)), dma((2,)), dma((2,)),
                dma((2, chips)), dma((2, chips)), dma((2, chips)), dma((2, chips)),
            ],
            compiler_params=pltpu.CompilerParams(collective_id=0, has_side_effects=True,
                                                 vmem_limit_bytes=56 * 1024 * 1024),
            name='attention_backward',
        )(*args)
        dk, dv, dq = pl.pallas_call(
            _write,
            out_shape=[jax.ShapeDtypeStruct((tokens, heads, dim), BF16)] * 3,
            in_specs=[pl.BlockSpec(memory_space=pltpu.VMEM)],
            out_specs=[pl.BlockSpec(memory_space=pl.ANY)] * 3,
            scratch_shapes=[dma((3,))],
            compiler_params=pltpu.CompilerParams(vmem_limit_bytes=8 * 1024 * 1024),
            name='write_gradients',
        )(pltpu.with_memory_space_constraint(grads, pltpu.VMEM))
        return tuple(x.reshape(batch, tokens, heads, dim) for x in (dq, dk, dv))

    return jax.shard_map(local, mesh=mesh, in_specs=(spec, spec, spec, spec, lspec, spec),
                         out_specs=(spec, spec, spec), check_vma=False)
```

```python
import functools

import jax
import jax.numpy as jnp
from jax import lax
from jax.experimental import pallas as pl
from jax.experimental.pallas import tpu as pltpu
from jax.sharding import PartitionSpec as P

F32 = jnp.float32
BF16 = jnp.bfloat16
MESH = pl.DeviceIdType.MESH
EARLY, LATE = 0, 1
K, V, Q, DO, O = range(5)


def _dot(a, b):
    return jnp.dot(a, b, preferred_element_type=F32)


def _dot_nt(a, b):
    return lax.dot_general(a, b, (((1,), (1,)), ((), ())), preferred_element_type=F32)


def _kernel(n, q_h, k_h, v_h, o_h, do_h, lse_h, outv,
            raw, lse_v, wide, send, ldsend, kv, qd, ld, kt, dqt, dqx, dkv, outs, outr,
            tokens_up, tokens_down, load_sem, lse_sem, kv_s, kv_r, qd_s, qd_r, ld_s, ld_r,
            fw_s, fw_r, fl_s, fl_r, dx_s, dx_r, og_s, og_r, oq_s, oq_r):
    chips = n // 2
    tokens, heads, dim = raw.shape[1:]
    c = tokens // 2
    lanes = wide.shape[-1]
    scale = dim ** -0.5
    me = lax.axis_index('cp')
    z = me // 2
    core = me % 2
    sib = me + 1 - 2 * core
    around = [d for k in range(1, chips // 2) for d in (chips - k, k)] + [chips // 2]

    def peer(chip):
        return {'cp': 2 * chip + core}

    barrier = pltpu.get_barrier_semaphore()
    above, below = peer((z + 1) % chips), peer((z + chips - 1) % chips)
    for near in (above, below):
        pl.semaphore_signal(barrier, inc=1, device_id=near, device_id_type=MESH)
    pl.semaphore_signal(barrier, inc=1, device_id={'cp': sib}, device_id_type=MESH)

    hbm = {K: k_h, V: v_h, Q: q_h, DO: do_h, O: o_h}

    def load(t, half):
        rows = pl.ds(half * c, c)
        return pltpu.make_async_copy(hbm[t].at[rows], raw.at[t, rows], load_sem.at[t, half])

    load(K, LATE).start()
    load(V, LATE).start()

    pl.semaphore_wait(barrier, 3)

    def pass_on(k):
        pl.semaphore_signal(tokens_up.at[k], inc=1, device_id=above, device_id_type=MESH)
        pl.semaphore_signal(tokens_down.at[k], inc=1, device_id=below, device_id_type=MESH)

    def hear(k):
        pl.semaphore_wait(tokens_up.at[k], 1)
        pl.semaphore_wait(tokens_down.at[k], 1)

    pass_on(1)
    for t in (Q, DO, O):
        load(t, LATE).start()
    for t in (K, V, Q, DO, O):
        load(t, EARLY).start()
    lse_load = pltpu.make_async_copy(lse_h, lse_v, lse_sem)
    lse_load.start()

    def spread(x):
        for l in range(dim // lanes):
            wide[0, l] = x[:, :, l * lanes:(l + 1) * lanes].reshape(c * heads, lanes)

    def head_rows(h):
        return pl.ds(h, c, stride=heads)

    def relayout(t, half, wait=True):
        if wait:
            load(t, half).wait()
        spread(raw[t, pl.ds(half * c, c)].astype(F32))
        for h in range(heads):
            for l in range(dim // lanes):
                send[half, t, h, :, pl.ds(l * lanes, lanes)] = wide[0, l, head_rows(h), :].astype(BF16)

    def copy_kv(half, d, slot):
        head = (z + d) % chips
        src, dst = send.at[half, pl.ds(K, 2), head], kv.at[half, :, slot]
        if isinstance(d, int) and d == 0:
            return pltpu.make_async_copy(src, dst, kv_r.at[half, slot])
        return pltpu.make_async_remote_copy(src, dst, kv_s.at[half, d], kv_r.at[half, slot],
                                            device_id=peer(head), device_id_type=MESH)

    def copy_qd(half, d, slot):
        head = (z + d) % chips
        src, dst = send.at[half, pl.ds(Q, 2), head], qd.at[half, :, 2 * slot + core]
        if isinstance(d, int) and d == 0:
            return pltpu.make_async_copy(src, dst, qd_r.at[half, slot])
        return pltpu.make_async_remote_copy(src, dst, qd_s.at[half, d], qd_r.at[half, slot],
                                            device_id=peer(head), device_id_type=MESH)

    def copy_ld(d, slot):
        head = (z + d) % chips
        src, dst = ldsend.at[head], ld.at[2 * slot + core]
        if isinstance(d, int) and d == 0:
            return pltpu.make_async_copy(src, dst, ld_r.at[slot])
        return pltpu.make_async_remote_copy(src, dst, ld_s.at[d], ld_r.at[slot],
                                            device_id=peer(head), device_id_type=MESH)

    def forward_qd(half, slot, parity):
        ref = qd.at[half, :, 2 * slot + parity]
        return pltpu.make_async_remote_copy(ref, ref, fw_s.at[half, slot], fw_r.at[half, slot],
                                            device_id={'cp': sib}, device_id_type=MESH)

    def forward_ld(slot, parity):
        ref = ld.at[2 * slot + parity]
        return pltpu.make_async_remote_copy(ref, ref, fl_s.at[slot], fl_r.at[slot],
                                            device_id={'cp': sib}, device_id_type=MESH)

    def exchange_dq(half):
        return pltpu.make_async_remote_copy(dqt.at[half, :, 1 - core], dqx.at[half], dx_s.at[half], dx_r.at[half],
                                            device_id={'cp': sib}, device_id_type=MESH)

    def copy_dkv(half, d, slot):
        chip = (z + d) % chips
        src, dst = outs.at[half, pl.ds(0, 2), chip], outr.at[half, pl.ds(0, 2), slot]
        if isinstance(d, int) and d == 0:
            return pltpu.make_async_copy(src, dst, og_r.at[half, slot])
        return pltpu.make_async_remote_copy(src, dst, og_s.at[half, d], og_r.at[half, slot],
                                            device_id=peer(chip), device_id_type=MESH)

    def copy_dq(half, d, slot):
        chip = (z + d) % chips
        src, dst = outs.at[half, 2, chip], outr.at[half, 2, slot]
        if isinstance(d, int) and d == 0:
            return pltpu.make_async_copy(src, dst, oq_r.at[half, slot])
        return pltpu.make_async_remote_copy(src, dst, oq_s.at[half, d], oq_r.at[half, slot],
                                            device_id=peer(chip), device_id_type=MESH)

    def start_all(make):
        for d in [0] + around:
            make(d, z).start()

    def start_all_low_first(make):
        @pl.when(z == 0)
        def _():
            make(0, z).start()

        @pl.when(z != 0)
        def _():
            make(chips - z, z).start()

        for d in [0] + around:
            @pl.when((z + d) % chips != 0)
            def _():
                make(d, z).start()

    def wait_from(make, d):
        if d == 0:
            make(0, z).wait()
        else:
            make(d, (z - d + chips) % chips).wait_recv()

    def wait_sent(make):
        for d in around:
            make(d, z).wait_send()

    relayout(K, LATE)
    relayout(V, LATE)
    copy_kv(LATE, 0, z).start()
    for k in range(1, chips // 2 + 1):
        if k > 1:
            hear(k - 1)
            if k < chips // 2:
                pass_on(k)
        for d in around:
            if min(d, chips - d) == k:
                copy_kv(LATE, d, z).start()
    relayout(Q, LATE)
    relayout(DO, LATE)
    start_all(functools.partial(copy_qd, LATE))
    lse_load.wait()
    for half in (LATE, EARLY):
        load(O, half).wait()
        if half == EARLY:
            load(DO, half).wait()
        rows = pl.ds(half * c, c)
        spread(raw[DO, rows].astype(F32) * raw[O, rows].astype(F32))
        for h in range(heads):
            prod = sum(wide[0, l, head_rows(h), :] for l in range(dim // lanes))
            ldsend[h, pl.ds(2 + half, 1), :] = jnp.sum(prod.T, axis=0, keepdims=True)
            ldsend[h, pl.ds(half, 1), :] = lse_v[pl.ds(h, 1), pl.ds(half * c, c)]
    start_all(copy_ld)

    relayout(K, EARLY)
    relayout(V, EARLY)
    start_all(functools.partial(copy_kv, EARLY))
    relayout(Q, EARLY)
    relayout(DO, EARLY, wait=False)
    start_all(functools.partial(copy_qd, EARLY))

    def clear(s, carry):
        for half in range(2):
            for p in range(2):
                dqt[half, s, p] = jnp.zeros((dim, c), F32)
                dkv[half, p, s] = jnp.zeros((c, dim), F32)
        return carry

    lax.fori_loop(0, chips, clear, 0)

    def tile(kh, qh, i, j, width, masked):
        k = kv[kh, 0, pl.ds(2 * i, 2)].reshape(2 * c, dim)
        v = kv[kh, 1, pl.ds(2 * i, 2)].reshape(2 * c, dim)
        first = width * j
        q = qd[qh, 0, pl.ds(first, width)].reshape(width * c, dim)
        do = qd[qh, 1, pl.ds(first, width)].reshape(width * c, dim)
        lse = jnp.concatenate([ld[first + w, pl.ds(qh, 1), :] for w in range(width)], axis=1)
        delta = jnp.concatenate([ld[first + w, pl.ds(2 + qh, 1), :] for w in range(width)], axis=1)
        p = jnp.exp(_dot_nt(k, q) * scale - lse)
        if masked:
            sign = 1 if kh == EARLY else -1
            row = lax.broadcasted_iota(jnp.int32, (2 * c, width * c), 0)
            col = lax.broadcasted_iota(jnp.int32, (2 * c, width * c), 1)
            kpos = jnp.where(row >= c, row - c + sign * 2 * c, row) + sign * (4 * i + core) * c
            qpos = jnp.where(col >= c, col - c + sign * c, col) + sign * first * c
            p = jnp.where(qpos >= kpos, p, 0.0)
        rows = pl.ds(2 * i, 2)
        dkv[kh, 1, rows] += _dot(p.astype(BF16), do).reshape(2, c, dim)
        ds = (p * (_dot_nt(v, do) - delta)).astype(BF16)
        dkv[kh, 0, rows] += _dot(ds, q).reshape(2, c, dim)
        dq = _dot(kt[...], ds)
        for w in range(width):
            dqt[qh, width // 2 * j + w // 2, w % 2] += dq[:, w * c:(w + 1) * c]

    def sweep(kh, qh, lo, hi, width, masked):
        def outer(i, carry):
            kt[...] = kv[kh, 0, pl.ds(2 * i, 2)].reshape(2 * c, dim).T

            def inner(j, carry):
                tile(kh, qh, i, j, width, masked)
                return carry

            lax.fori_loop(lo(i), hi(i), inner, 0)
            return carry

        lax.fori_loop(0, chips // 2, outer, 0)

    def receive_qd(half):
        for d in [0] + around:
            wait_from(functools.partial(copy_qd, half), d)
            forward_qd(half, (z - d + chips) % chips, core).start()

    def receive_forwarded(half):
        for s in range(chips):
            forward_qd(half, s, 1 - core).wait_recv()

    def receive_kv(half):
        for d in [0] + around:
            wait_from(functools.partial(copy_kv, half), d)

    def round_dkv(half):
        def one(s, carry):
            outs[half, 0, s] = (dkv[half, 0, s] * scale).astype(BF16)
            outs[half, 1, s] = dkv[half, 1, s].astype(BF16)
            return carry

        lax.fori_loop(0, chips, one, 0)

    def round_dq(half):
        def one(s, carry):
            outs[half, 2, s] = ((dqt[half, s, core] + dqx[half, s]) * scale).astype(BF16).T
            return carry

        lax.fori_loop(0, chips, one, 0)

    receive_qd(LATE)
    for d in [0] + around:
        wait_from(copy_ld, d)
        forward_ld((z - d + chips) % chips, core).start()
    receive_kv(LATE)
    receive_forwarded(LATE)
    for s in range(chips):
        forward_ld(s, 1 - core).wait_recv()
    sweep(LATE, LATE, lambda i: 0, lambda i: 2 * i + 2, 2, True)
    round_dkv(LATE)
    start_all(functools.partial(copy_dkv, LATE))

    receive_kv(EARLY)
    sweep(EARLY, LATE, lambda i: 0, lambda i: chips // 2, 4, False)
    exchange_dq(LATE).start()
    receive_qd(EARLY)
    exchange_dq(LATE).wait()
    round_dq(LATE)
    start_all(functools.partial(copy_dq, LATE))

    receive_forwarded(EARLY)
    sweep(EARLY, EARLY, lambda i: 2 * i, lambda i: chips, 2, True)
    round_dkv(EARLY)
    exchange_dq(EARLY).start()
    start_all_low_first(functools.partial(copy_dkv, EARLY))
    exchange_dq(EARLY).wait()
    round_dq(EARLY)
    start_all_low_first(functools.partial(copy_dq, EARLY))

    def gather(make, half, ts):
        for d in [0] + around[::-1]:
            wait_from(functools.partial(make, half), d)
            h = (z - d + chips) % chips
            for t in ts:
                for l in range(dim // lanes):
                    wide[t, l, head_rows(h), :] = outr[half, t, h, :, pl.ds(l * lanes, lanes)].astype(F32)
        for t in ts:
            for l in range(dim // lanes):
                outv[t, pl.ds(half * c, c), :, pl.ds(l * lanes, lanes)] = (
                    wide[t, l].reshape(c, heads, lanes).astype(BF16))

    for half in (LATE, EARLY):
        gather(copy_dkv, half, (0, 1))
        gather(copy_dq, half, (2,))

    for half in (LATE, EARLY):
        for make in (copy_kv, copy_qd, copy_dkv, copy_dq):
            wait_sent(functools.partial(make, half))
        for s in range(chips):
            forward_qd(half, s, core).wait_send()
    wait_sent(copy_ld)
    for s in range(chips):
        forward_ld(s, core).wait_send()


def _write(x, dk, dv, dq, sem):
    copies = [pltpu.make_async_copy(x.at[t], out, sem.at[t]) for t, out in enumerate((dk, dv, dq))]
    for copy in copies:
        copy.start()
    for copy in copies:
        copy.wait()


def solution(mesh):
    n = mesh.shape['cp']
    spec = P('data', 'cp', None, None)
    lspec = P('data', None, 'cp')

    def local(q, k, v, o, lse, do):
        batch, tokens, heads, dim = q.shape
        chips = n // 2
        assert batch == 1 and heads == chips
        c = tokens // 2
        dma = pltpu.SemaphoreType.DMA
        args = [x.reshape(tokens, heads, dim) for x in (q, k, v, o, do)] + [lse.reshape(heads, tokens)]
        grads = pl.pallas_call(
            functools.partial(_kernel, n),
            out_shape=pltpu.VMEM((3, tokens, heads, dim), BF16),
            in_specs=[pl.BlockSpec(memory_space=pl.ANY)] * 6,
            out_specs=pl.BlockSpec(memory_space=pltpu.VMEM),
            scratch_shapes=[
                pltpu.VMEM((5, tokens, heads, dim), BF16),
                pltpu.VMEM((heads, tokens), F32),
                pltpu.VMEM((3, dim // 128, c * heads, 128), F32),
                pltpu.VMEM((2, 4, heads, c, dim), BF16),
                pltpu.VMEM((heads, 4, c), F32),
                pltpu.VMEM((2, 2, chips, c, dim), BF16),
                pltpu.VMEM((2, 2, n, c, dim), BF16),
                pltpu.VMEM((n, 4, c), F32),
                pltpu.VMEM((dim, 2 * c), BF16),
                pltpu.VMEM((2, chips, 2, dim, c), F32),
                pltpu.VMEM((2, chips, dim, c), F32),
                pltpu.VMEM((2, 2, chips, c, dim), F32),
                pltpu.VMEM((2, 3, chips, c, dim), BF16),
                pltpu.VMEM((2, 3, heads, c, dim), BF16),
                pltpu.SemaphoreType.REGULAR((chips // 2,)), pltpu.SemaphoreType.REGULAR((chips // 2,)),
                dma((5, 2)), dma,
                dma((2, chips)), dma((2, chips)), dma((2, chips)), dma((2, chips)), dma((chips,)), dma((chips,)),
                dma((2, chips)), dma((2, chips)), dma((chips,)), dma((chips,)), dma((2,)), dma((2,)),
                dma((2, chips)), dma((2, chips)), dma((2, chips)), dma((2, chips)),
            ],
            compiler_params=pltpu.CompilerParams(collective_id=0, has_side_effects=True,
                                                 vmem_limit_bytes=56 * 1024 * 1024),
            name='attention_backward',
        )(*args)
        dk, dv, dq = pl.pallas_call(
            _write,
            out_shape=[jax.ShapeDtypeStruct((tokens, heads, dim), BF16)] * 3,
            in_specs=[pl.BlockSpec(memory_space=pltpu.VMEM)],
            out_specs=[pl.BlockSpec(memory_space=pl.ANY)] * 3,
            scratch_shapes=[dma((3,))],
            compiler_params=pltpu.CompilerParams(vmem_limit_bytes=8 * 1024 * 1024),
            name='write_gradients',
        )(pltpu.with_memory_space_constraint(grads, pltpu.VMEM))
        return tuple(x.reshape(batch, tokens, heads, dim) for x in (dq, dk, dv))

    return jax.shard_map(local, mesh=mesh, in_specs=(spec, spec, spec, spec, lspec, spec),
                         out_specs=(spec, spec, spec), check_vma=False)
```
